32 devices in a mesh: clusters: 4 (over y, x), members: 8 (over z, core).
Axes of the slice: x: 2, y: 2, z: 4, core: 2. Of those that a mesh axis runs over, the one named last changes fastest.
Arguments:
- embeddings: float32 [16384, 1024], P(('clusters', 'members')), parts along dimension 0, as said below
- member_order: int32 [16384], P(('clusters', 'members')), parts along dimension 0, may hold values from 0 to 4095, each once
- threshold: float32 [4], P('clusters'), parts along dimension 0, may hold values from 0.25 to 0.5
Outputs:
- best_similarity: float32 [16384], P(('clusters', 'members')), parts along dimension 0
- excess: float32 [16384], P(('clusters', 'members')), parts along dimension 0
The draws below stay inside these ranges and needn't reach their ends.
There are 4 independent parts, one for each index of `clusters`. The reference program is written for one: setup_inputs(seed, part) draws one part's arguments, and reference() takes and returns one part's arrays. A program takes and returns all parts, laid end to end along the dimension named above; each array names one. Nothing has to cross between parts.
Inputs may be any that keep to these rules, and one draw needn't show every extreme that they name: member_order holds each of 0 to 4095 once. real-valued embeddings.
All inputs are finite; a program needn't handle non-finite values.
Results may differ from the reference program's by a relative error of at most 0.00051.
Values may be sent and summed in bfloat16 or wider, within the bound.
A program may use at most 128 MiB of HBM per device.

```python
import math
import jax
import jax.numpy as jnp
from jax import lax

E = 1024
MEMBERS = 4096


def draw_embeddings(key, part):
    keys = jax.random.split(key, 4)
    groups = MEMBERS // 4
    protos = jax.random.normal(keys[0], (groups, E), jnp.float32)
    group_id = jax.random.randint(keys[1], (MEMBERS,), 0, groups)
    mixing = jax.random.uniform(keys[2], (MEMBERS, 1), jnp.float32, 0.0, 2.5)
    noise = jax.random.normal(keys[3], (MEMBERS, E), jnp.float32)
    values = protos[group_id] * mixing + noise
    return values.astype(jnp.float32)


def setup_inputs(seed: int = 0, part: int = 0) -> dict:
    key_list = jax.random.split(jax.random.key(seed), 4)
    part_keys = jax.random.split(jax.random.fold_in(key_list[3], part), 4)
    return {
        "embeddings": draw_embeddings(jax.random.fold_in(jax.random.fold_in(key_list[3], part), 71), part),
        "member_order": jax.random.permutation(part_keys[1], MEMBERS).astype(jnp.int32),
        "threshold": jnp.clip(jax.random.uniform(part_keys[2], (1,), jnp.float32, 0.25, 0.5), 0.25, 0.5),
    }


def reference(embeddings, member_order, threshold):
    unit = (embeddings * lax.rsqrt(lax.optimization_barrier(jnp.sum(embeddings * embeddings, axis=1, keepdims=True)) + 1e-06)).astype(jnp.bfloat16)
    total = unit.shape[0]
    block = math.gcd(total, 512)
    rows = unit.reshape(total // block, block, unit.shape[1])
    orders = member_order.reshape(total // block, block)

    def one_block(pair):
        part_rows, part_order = pair
        sim = jnp.dot(part_rows, unit.T, preferred_element_type=jnp.float32)
        mask = member_order[None, :] < part_order[:, None]
        picked = jnp.where(mask, sim, jnp.float32(-1.0))
        return jnp.maximum(lax.optimization_barrier(jnp.max(picked, axis=1)), jnp.float32(-1.0))
    best = lax.map(one_block, (rows, orders)).reshape(total)
    excess = jnp.maximum(best - threshold[0], jnp.float32(0.0))
    return (best, excess)
```

```python
import functools

import jax
import jax.numpy as jnp
from jax import lax
from jax.experimental import pallas as pl
from jax.experimental.pallas import tpu as pltpu
from jax.sharding import PartitionSpec as P

MESH = pl.DeviceIdType.MESH
LANES = 128
SUBS = 8
COLS = 256


def from_behind(array, axis, by):
    size = lax.axis_size(axis)
    return lax.ppermute(array, axis, [(i, (i + by) % size) for i in range(size)])


def block_scores(unit, other):
    return lax.dot_general(
        unit, other, (((1,), (1,)), ((), ())), preferred_element_type=jnp.float32
    )


def ring(embeddings, member_order, threshold):
    unit = (
        embeddings * lax.rsqrt(jnp.sum(embeddings * embeddings, axis=1, keepdims=True) + 1e-06)
    ).astype(jnp.bfloat16)
    floor_value = jnp.float32(-1.0)
    start_best = jnp.full((unit.shape[0],), -1.0, jnp.float32)
    steps_half = lax.axis_size("members") // 2
    scores = block_scores(unit, unit)
    mask = member_order[None, :] < member_order[:, None]
    best = jnp.maximum(start_best, jnp.max(jnp.where(mask, scores, floor_value), axis=1))

    def one_step(step, carry):
        held_unit, held_order, column_best, row_best = carry
        held_unit, held_order = from_behind((held_unit, held_order), "members", 1)
        column_best = from_behind(column_best, "members", 1)
        scores = block_scores(unit, held_unit)
        row_mask = held_order[None, :] < member_order[:, None]
        row_best = jnp.maximum(row_best, jnp.max(jnp.where(row_mask, scores, floor_value), axis=1))
        column_mask = member_order[:, None] < held_order[None, :]
        column_best = jnp.maximum(
            column_best, jnp.max(jnp.where(column_mask, scores, floor_value), axis=0)
        )
        return (held_unit, held_order, column_best, row_best)

    carry = (unit, member_order, start_best, best)
    carry = lax.fori_loop(0, steps_half, one_step, carry)
    returned = from_behind(carry[2], "members", -steps_half)
    best = jnp.maximum(carry[3], returned)
    excess = jnp.maximum(best - threshold[0], jnp.float32(0.0))
    return (best, excess)


def hub_kernel(emb, order, threshold, best_out, excess_out, held, relay, order_row, order_column,
               row_best, column_best, stage, arrived, send_sem, stream_sem, small_sem):
    n = emb.shape[0]
    half = n // 2
    piece = n // SUBS
    unit_rows = LANES
    units = n // unit_rows
    per_unit = SUBS // units
    small = unit_rows // 2 // per_unit
    OWN, MATE, P3, P3O, P0, P1 = [i * n for i in range(6)]
    RX, RY = 0, half

    cluster = lax.axis_index("clusters")
    member = lax.axis_index("members")
    members = lax.axis_size("members")
    chips = members // 2
    core = lax.rem(member, 2)
    z = member // 2
    cx = lax.rem(cluster, 2)
    cy = cluster // 2
    flip = lax.rem(cx + cy, 2)
    p = z + flip * (chips - 1 - 2 * z)
    x_peer = (cluster + 1 - 2 * cx, member)
    y_peer = (cluster + 2 - 4 * cy, member)

    def role(r, other_core=False):
        zz = r + flip * (chips - 1 - 2 * r)
        cc = 1 - core if other_core else core
        return (cluster, zz * 2 + cc)

    mate = (cluster, z * 2 + 1 - core)

    barrier = pltpu.get_barrier_semaphore()
    for step in range(1, 8):
        pl.semaphore_signal(
            barrier, inc=1, device_id=(cluster, lax.rem(member + step, members)), device_id_type=MESH
        )
    for peer in (x_peer, y_peer):
        pl.semaphore_signal(barrier, inc=1, device_id=peer, device_id_type=MESH)

    def normalise(i, _):
        rows = pl.ds(pl.multiple_of(i * 64, 64), 64)
        e = emb[rows, :]
        total = jnp.sum(e * e, axis=1, keepdims=True)
        held[rows, :] = (e * lax.rsqrt(total + 1e-06)).astype(jnp.bfloat16)
        return 0

    lax.fori_loop(0, n // 64, normalise, 0)
    order_row[:, pl.ds(OWN, n)] = order[...]
    row_best[...] = jnp.full(row_best.shape, -1.0, jnp.float32)
    column_best[...] = jnp.full(column_best.shape, -1.0, jnp.float32)

    def put_order_column(at):
        o = order_row[:, pl.ds(at, n)]
        order_column[pl.ds(at, n), :] = jnp.broadcast_to(o, (LANES, n)).T

    put_order_column(OWN)
    pl.semaphore_wait(barrier, 9)

    sent = []

    def send(src, dst, sem, peer):
        copy = pltpu.make_async_remote_copy(
            src_ref=src, dst_ref=dst, send_sem=send_sem.at[len(sent)], recv_sem=sem,
            device_id=peer, device_id_type=MESH,
        )
        copy.start()
        sent.append(copy)

    def receive(dst, sem):
        pltpu.make_async_remote_copy(
            src_ref=dst, dst_ref=dst, send_sem=send_sem.at[0], recv_sem=sem,
            device_id=mate, device_id_type=MESH,
        ).wait_recv()

    def rows_of(at, size):
        return held.at[pl.ds(at, size), :]

    def orders_of(at):
        return order_row.at[:, pl.ds(at, n)]

    def send_order(to, sem_index, peer):
        send(orders_of(OWN), orders_of(to), small_sem.at[sem_index], peer)

    def receive_order(at, sem_index):
        receive(orders_of(at), small_sem.at[sem_index])

    def finish():
        for copy in sent:
            copy.wait_send()
        sent.clear()

    def pairs(row0, rows, col0, cols, columns_too=True):
        tile = 256

        def one(i, _):
            r = pl.ds(pl.multiple_of(row0 + i * tile, tile), tile)
            s = block_scores(held[r, :], held[pl.ds(col0, cols), :])
            oc = order_column[r, :]
            best = row_best[r, :]
            for c in range(0, cols, LANES):
                part = s[:, c:c + LANES]
                o = order_row[:, pl.ds(col0 + c, LANES)]
                earlier = o < oc
                best = jnp.maximum(best, jnp.where(earlier, part, -1.0))
                if columns_too:
                    other = jnp.where(earlier, -1.0, part).reshape(tile // 8, 8, LANES)
                    at = pl.ds(col0 + c, LANES)
                    column_best[:, at] = jnp.maximum(column_best[:, at], jnp.max(other, axis=0))
            row_best[r, :] = best
            return 0

        lax.fori_loop(0, rows // tile, one, 0)

    def row_result(at):
        return jnp.max(row_best[pl.ds(at, n), :].T, axis=0, keepdims=True)

    def column_result(at):
        return jnp.max(column_best[:, pl.ds(at, n)], axis=0, keepdims=True)

    def send_result(slot, value, to, peer):
        stage[slot] = value
        send(stage.at[slot], arrived.at[to], small_sem.at[8 + to], peer)

    def take_result(slot):
        receive(arrived.at[slot], small_sem.at[8 + slot])
        return arrived[slot]

    def put(best):
        best_out[...] = best
        excess_out[...] = jnp.maximum(best - threshold[0], jnp.float32(0.0))

    def exchange():
        send_order(MATE, 0, mate)
        send(rows_of(OWN, n), rows_of(MATE, n), small_sem.at[5], mate)

    def local():
        for c in range(0, n, COLS):
            pairs(OWN, n, OWN + c, COLS, False)
        receive_order(MATE, 0)
        receive(rows_of(MATE, n), small_sem.at[5])
        for c in range(0, n, COLS):
            pairs(OWN, n, MATE + c, COLS, False)

    def x_rows(s):
        return (s // per_unit) * unit_rows + (s % per_unit) * small

    def y_rows(s):
        return x_rows(s) + unit_rows // 2

    @pl.when(p == 0)
    def _():
        send_order(P0, 1, role(1))
        send_order(P0, 1, role(2))
        for s in range(SUBS):
            send(rows_of(OWN + s * piece, piece), rows_of(P0 + s * piece, piece), stream_sem.at[0, s], role(1))
        exchange()
        local()
        best = row_result(OWN)
        best = jnp.maximum(best, take_result(1))
        put(jnp.maximum(best, take_result(2)))
        finish()

    @pl.when(p == 3)
    def _():
        send_order(P3, 3, role(2))
        send_order(P3O, 4, role(2, True))
        for s in range(SUBS):
            send(rows_of(OWN + s * piece, piece), rows_of(P3 + s * piece, piece), stream_sem.at[3, s], role(2))
        exchange()
        local()
        best = row_result(OWN)
        best = jnp.maximum(best, take_result(1))
        put(jnp.maximum(best, take_result(2)))
        finish()

    def relay_piece(base, s):
        return relay.at[pl.ds(base + s * small, small), :]

    @pl.when(p == 1)
    def _():
        send_order(P1, 2, role(2))
        for s in range(SUBS):
            send(rows_of(OWN + x_rows(s), small), relay_piece(RX, s), stream_sem.at[5, s], x_peer)
            send(rows_of(OWN + y_rows(s), small), relay_piece(RY, s), stream_sem.at[6, s], y_peer)
        exchange()
        local()
        put_order_column(MATE)
        receive_order(P0, 1)
        lag = 1
        for s in range(SUBS + lag):
            if s < SUBS:
                at = rows_of(P0 + s * piece, piece)
                receive(at, stream_sem.at[0, s])
                send(at, at, stream_sem.at[0, s], role(2))
            if s >= lag:
                k = s - lag
                receive(relay_piece(RX, k), stream_sem.at[5, k])
                send(relay_piece(RX, k), rows_of(P1 + x_rows(k), small), stream_sem.at[1, k], x_peer)
                receive(relay_piece(RY, k), stream_sem.at[6, k])
                send(relay_piece(RY, k), rows_of(P1 + y_rows(k), small), stream_sem.at[2, k], y_peer)
            if s % 4 == 3 and s < SUBS:
                pairs(OWN, 2 * n, P0 + (s - 3) * piece, 4 * piece)
        send_result(0, row_result(MATE), 0, mate)
        send_result(1, column_result(P0), 1, role(0))
        best = row_result(OWN)
        best = jnp.maximum(best, take_result(0))
        put(jnp.maximum(best, take_result(2)))
        finish()

    @pl.when(p == 2)
    def _():
        exchange()
        local()
        put_order_column(MATE)
        receive_order(P3, 3)
        put_order_column(P3)
        receive_order(P3O, 4)
        put_order_column(P3O)
        receive_order(P0, 1)
        receive_order(P1, 2)

        def take_unit(u):
            for s in range(u * per_unit, (u + 1) * per_unit):
                receive(rows_of(P0 + s * piece, piece), stream_sem.at[0, s])
                receive(rows_of(P1 + x_rows(s), small), stream_sem.at[1, s])
                receive(rows_of(P1 + y_rows(s), small), stream_sem.at[2, s])

        early = units - 2
        for s in range(SUBS):
            receive(relay_piece(RX, s), stream_sem.at[5, s])
            send(relay_piece(RX, s), relay_piece(RX, s), stream_sem.at[5, s], role(1))
            receive(relay_piece(RY, s), stream_sem.at[6, s])
            send(relay_piece(RY, s), relay_piece(RY, s), stream_sem.at[6, s], role(1))
            at = rows_of(P3 + s * piece, piece)
            receive(at, stream_sem.at[3, s])
            send(at, rows_of(P3O + s * piece, piece), stream_sem.at[4, s], mate)
            if s % per_unit == per_unit - 1:
                u = s // per_unit
                pairs(OWN, 2 * n, P3 + u * unit_rows, unit_rows)
                u = u - 2
                if u >= 0:
                    take_unit(u)
                    pairs(OWN, 2 * n, P0 + u * unit_rows, unit_rows)
                    pairs(OWN, 2 * n, P1 + u * unit_rows, unit_rows)
        for s in range(SUBS):
            receive(rows_of(P3O + s * piece, piece), stream_sem.at[4, s])
        pairs(P3, 2 * n, P0, early * unit_rows)
        pairs(P3, 2 * n, P1, early * unit_rows)
        for u in range(early, units):
            take_unit(u)
            pairs(OWN, 4 * n, P0 + u * unit_rows, unit_rows)
            pairs(OWN, 4 * n, P1 + u * unit_rows, unit_rows)
        send_result(0, column_result(P0), 2, role(0))
        send_result(1, column_result(P1), 2, role(1))
        send_result(2, jnp.maximum(column_result(P3), row_result(P3)), 1, role(3))
        send_result(3, row_result(P3O), 2, role(3, True))
        send_result(4, row_result(MATE), 0, mate)
        best = row_result(OWN)
        put(jnp.maximum(best, take_result(0)))
        finish()


def hub(embeddings, member_order, threshold):
    n, width = embeddings.shape
    vmem = pl.BlockSpec(memory_space=pltpu.VMEM)
    best, excess = pl.pallas_call(
        hub_kernel,
        out_shape=[jax.ShapeDtypeStruct((1, n), jnp.float32)] * 2,
        in_specs=[vmem, vmem, pl.BlockSpec(memory_space=pltpu.SMEM)],
        out_specs=[vmem, vmem],
        scratch_shapes=[
            pltpu.VMEM((6 * n, width), jnp.bfloat16),
            pltpu.VMEM((n, width), jnp.bfloat16),
            pltpu.VMEM((1, 6 * n), jnp.int32),
            pltpu.VMEM((4 * n, LANES), jnp.int32),
            pltpu.VMEM((4 * n, LANES), jnp.float32),
            pltpu.VMEM((8, 6 * n), jnp.float32),
            pltpu.VMEM((5, 1, n), jnp.float32),
            pltpu.VMEM((3, 1, n), jnp.float32),
            pltpu.SemaphoreType.DMA((6 * SUBS + 16,)),
            pltpu.SemaphoreType.DMA((7, SUBS)),
            pltpu.SemaphoreType.DMA((11,)),
        ],
        compiler_params=pltpu.CompilerParams(collective_id=0, has_side_effects=True),
    )(embeddings, member_order.reshape(1, n), threshold)
    return best.reshape(n), excess.reshape(n)


def solution(mesh):
    lines = mesh.shape["clusters"] == 4 and mesh.shape["members"] == 8
    placed = (P(("clusters", "members"), None), P(("clusters", "members")), P("clusters"))
    return jax.shard_map(
        hub if lines else ring,
        mesh=mesh,
        in_specs=placed,
        out_specs=(P(("clusters", "members")), P(("clusters", "members"))),
        check_vma=False,
    )
```

```python
import jax
import jax.numpy as jnp
from jax import lax
from jax.experimental import pallas as pl
from jax.experimental.pallas import tpu as pltpu
from jax.sharding import PartitionSpec as P

MESH = pl.DeviceIdType.MESH
LANES = 128
SUBS = 8
TILE = 512


def from_behind(array, axis, by):
    size = lax.axis_size(axis)
    return lax.ppermute(array, axis, [(i, (i + by) % size) for i in range(size)])


def block_scores(unit, other):
    return lax.dot_general(
        unit, other, (((1,), (1,)), ((), ())), preferred_element_type=jnp.float32
    )


def ring(embeddings, member_order, threshold):
    unit = (
        embeddings * lax.rsqrt(jnp.sum(embeddings * embeddings, axis=1, keepdims=True) + 1e-06)
    ).astype(jnp.bfloat16)
    floor_value = jnp.float32(-1.0)
    start_best = jnp.full((unit.shape[0],), -1.0, jnp.float32)
    steps_half = lax.axis_size("members") // 2
    scores = block_scores(unit, unit)
    mask = member_order[None, :] < member_order[:, None]
    best = jnp.maximum(start_best, jnp.max(jnp.where(mask, scores, floor_value), axis=1))

    def one_step(step, carry):
        held_unit, held_order, column_best, row_best = carry
        held_unit, held_order = from_behind((held_unit, held_order), "members", 1)
        column_best = from_behind(column_best, "members", 1)
        scores = block_scores(unit, held_unit)
        row_mask = held_order[None, :] < member_order[:, None]
        row_best = jnp.maximum(row_best, jnp.max(jnp.where(row_mask, scores, floor_value), axis=1))
        column_mask = member_order[:, None] < held_order[None, :]
        column_best = jnp.maximum(
            column_best, jnp.max(jnp.where(column_mask, scores, floor_value), axis=0)
        )
        return (held_unit, held_order, column_best, row_best)

    carry = (unit, member_order, start_best, best)
    carry = lax.fori_loop(0, steps_half, one_step, carry)
    returned = from_behind(carry[2], "members", -steps_half)
    best = jnp.maximum(carry[3], returned)
    excess = jnp.maximum(best - threshold[0], jnp.float32(0.0))
    return (best, excess)


def hub_kernel(emb, order, best_out, held, relay, order_row, order_column,
               row_best, column_best, stage, arrived, send_sem, stream_sem, small_sem):
    n = emb.shape[0]
    half = n // 2
    piece = n // SUBS
    unit_rows = LANES
    units = n // unit_rows
    per_unit = SUBS // units
    small = unit_rows // 2 // per_unit
    OWN, MATE, P3, P3O, P0, P1 = [i * n for i in range(6)]
    MEET = P0
    RX, RY = 0, half

    cluster = lax.axis_index("clusters")
    member = lax.axis_index("members")
    members = lax.axis_size("members")
    chips = members // 2
    core = lax.rem(member, 2)
    z = member // 2
    cx = lax.rem(cluster, 2)
    cy = cluster // 2
    flip = lax.rem(cx + cy, 2)
    p = z + flip * (chips - 1 - 2 * z)
    x_peer = (cluster + 1 - 2 * cx, member)
    y_peer = (cluster + 2 - 4 * cy, member)

    def role(r, other_core=False):
        zz = r + flip * (chips - 1 - 2 * r)
        cc = 1 - core if other_core else core
        return (cluster, zz * 2 + cc)

    mate = (cluster, z * 2 + 1 - core)

    barrier = pltpu.get_barrier_semaphore()
    greets = (
        (mate, role(1), role(2)),
        (mate, role(0), role(2), x_peer, y_peer),
        (mate, role(0), role(1), role(3), role(3, True), x_peer, y_peer),
        (mate, role(2), role(2, True)),
    )
    for r, peers in enumerate(greets):
        @pl.when(p == r)
        def _():
            for peer in peers:
                pl.semaphore_signal(barrier, inc=1, device_id=peer, device_id_type=MESH)

    def normalise(i, _):
        rows = pl.ds(pl.multiple_of(i * 64, 64), 64)
        e = emb[rows, :]
        total = jnp.sum(e * e, axis=1, keepdims=True)
        held[rows, :] = (e * lax.rsqrt(total + 1e-06)).astype(jnp.bfloat16)
        return 0

    lax.fori_loop(0, n // 64, normalise, 0)
    order_row[:, pl.ds(OWN, n)] = order[...]
    row_best[...] = jnp.full(row_best.shape, -1.0, jnp.float32)
    column_best[...] = jnp.full(column_best.shape, -1.0, jnp.float32)

    def put_order_column(at):
        o = order_row[:, pl.ds(at, n)]
        order_column[pl.ds(at, n), :] = jnp.broadcast_to(o, (LANES, n)).T

    put_order_column(OWN)
    for r, peers in enumerate(greets):
        @pl.when(p == r)
        def _():
            pl.semaphore_wait(barrier, len(peers))

    sent = []

    def send(src, dst, sem, peer):
        copy = pltpu.make_async_remote_copy(
            src_ref=src, dst_ref=dst, send_sem=send_sem.at[len(sent)], recv_sem=sem,
            device_id=peer, device_id_type=MESH,
        )
        copy.start()
        sent.append(copy)

    def receive(dst, sem):
        pltpu.make_async_remote_copy(
            src_ref=dst, dst_ref=dst, send_sem=send_sem.at[0], recv_sem=sem,
            device_id=mate, device_id_type=MESH,
        ).wait_recv()

    def rows_of(at, size):
        return held.at[pl.ds(at, size), :]

    def orders_of(at):
        return order_row.at[:, pl.ds(at, n)]

    def send_order(to, sem_index, peer):
        send(orders_of(OWN), orders_of(to), small_sem.at[sem_index], peer)

    def receive_order(at, sem_index):
        receive(orders_of(at), small_sem.at[sem_index])

    def finish():
        for copy in sent:
            copy.wait_send()
        sent.clear()

    def pairs(row0, rows, col0, members_at, columns_too=True):
        def one(i, _):
            r = pl.ds(pl.multiple_of(row0 + i * TILE, TILE), TILE)
            s = block_scores(held[r, :], held[pl.ds(col0, len(members_at) * LANES), :])
            oc = order_column[r, :]
            best = row_best[r, :]
            for c, at in enumerate(members_at):
                part = s[:, c * LANES:(c + 1) * LANES]
                at = pl.ds(at, LANES)
                earlier = order_row[:, at] < oc
                best = jnp.maximum(best, jnp.where(earlier, part, -1.0))
                if columns_too:
                    other = jnp.where(earlier, -1.0, part).reshape(TILE // 8, 8, LANES)
                    column_best[:, at] = jnp.maximum(column_best[:, at], jnp.max(other, axis=0))
            row_best[r, :] = best
            return 0

        lax.fori_loop(0, rows // TILE, one, 0)

    def meet(row0, rows, u):
        pairs(row0, rows, MEET + 2 * u * unit_rows, (P0 + u * unit_rows, P1 + u * unit_rows))

    def row_result(at):
        return jnp.max(row_best[pl.ds(at, n), :].T, axis=0, keepdims=True)

    def column_result(at):
        return jnp.max(column_best[:, pl.ds(at, n)], axis=0, keepdims=True)

    def send_result(slot, value, to, peer):
        stage[slot] = value
        send(stage.at[slot], arrived.at[to], small_sem.at[8 + to], peer)

    def take_result(slot):
        receive(arrived.at[slot], small_sem.at[8 + slot])
        return arrived[slot]

    def put(best):
        best_out[...] = best

    def exchange():
        send_order(MATE, 0, mate)
        send(rows_of(OWN, n), rows_of(MATE, n), small_sem.at[5], mate)

    def local():
        for c in range(0, n, 2 * LANES):
            pairs(OWN, n, OWN + c, (OWN + c, OWN + c + LANES), False)
        receive_order(MATE, 0)
        receive(rows_of(MATE, n), small_sem.at[5])
        for c in range(0, n, 2 * LANES):
            pairs(OWN, n, MATE + c, (MATE + c, MATE + c + LANES), False)

    def x_rows(s):
        return (s // per_unit) * unit_rows + (s % per_unit) * small

    def y_rows(s):
        return x_rows(s) + unit_rows // 2

    def p0_piece(s):
        at = s * piece
        return rows_of(MEET + 2 * (at - at % unit_rows) + at % unit_rows, piece)

    def p1_piece(at):
        return rows_of(MEET + 2 * (at - at % unit_rows) + unit_rows + at % unit_rows, small)

    @pl.when(p == 0)
    def _():
        send_order(P0, 1, role(1))
        send_order(P0, 1, role(2))
        for s in range(SUBS):
            send(rows_of(OWN + s * piece, piece), p0_piece(s), stream_sem.at[0, s], role(1))
        exchange()
        local()
        best = row_result(OWN)
        best = jnp.maximum(best, take_result(1))
        put(jnp.maximum(best, take_result(2)))
        finish()

    @pl.when(p == 3)
    def _():
        send_order(P3, 3, role(2))
        send_order(P3O, 4, role(2, True))
        for s in range(SUBS):
            send(rows_of(OWN + s * piece, piece), rows_of(P3 + s * piece, piece), stream_sem.at[3, s], role(2))
        exchange()
        local()
        best = row_result(OWN)
        best = jnp.maximum(best, take_result(1))
        put(jnp.maximum(best, take_result(2)))
        finish()

    def relay_piece(base, s):
        return relay.at[pl.ds(base + s * small, small), :]

    @pl.when(p == 1)
    def _():
        send_order(P1, 2, role(2))
        for s in range(SUBS):
            send(rows_of(OWN + x_rows(s), small), relay_piece(RX, s), stream_sem.at[5, s], x_peer)
            send(rows_of(OWN + y_rows(s), small), relay_piece(RY, s), stream_sem.at[6, s], y_peer)
        exchange()
        local()
        put_order_column(MATE)
        receive_order(P0, 1)
        lag = 1
        for s in range(SUBS + lag):
            if s < SUBS:
                at = p0_piece(s)
                receive(at, stream_sem.at[0, s])
                send(at, at, stream_sem.at[0, s], role(2))
            if s >= lag:
                k = s - lag
                receive(relay_piece(RX, k), stream_sem.at[5, k])
                send(relay_piece(RX, k), p1_piece(x_rows(k)), stream_sem.at[1, k], x_peer)
                receive(relay_piece(RY, k), stream_sem.at[6, k])
                send(relay_piece(RY, k), p1_piece(y_rows(k)), stream_sem.at[2, k], y_peer)
                if k % per_unit == per_unit - 1:
                    u = k // per_unit
                    at = P0 + u * unit_rows
                    pairs(OWN, 2 * n, MEET + 2 * u * unit_rows, (at,))
        send_result(0, row_result(MATE), 0, mate)
        send_result(1, column_result(P0), 1, role(0))
        best = row_result(OWN)
        best = jnp.maximum(best, take_result(0))
        put(jnp.maximum(best, take_result(2)))
        finish()

    @pl.when(p == 2)
    def _():
        exchange()
        local()
        put_order_column(MATE)
        receive_order(P3, 3)
        put_order_column(P3)
        receive_order(P3O, 4)
        put_order_column(P3O)
        receive_order(P0, 1)
        receive_order(P1, 2)

        def take_unit(u):
            for s in range(u * per_unit, (u + 1) * per_unit):
                receive(p0_piece(s), stream_sem.at[0, s])
                receive(p1_piece(x_rows(s)), stream_sem.at[1, s])
                receive(p1_piece(y_rows(s)), stream_sem.at[2, s])

        early = units // 2
        for s in range(SUBS):
            for k in range(2 * s, min(2 * s + 2, SUBS)):
                receive(relay_piece(RX, k), stream_sem.at[5, k])
                send(relay_piece(RX, k), relay_piece(RX, k), stream_sem.at[5, k], role(1))
                receive(relay_piece(RY, k), stream_sem.at[6, k])
                send(relay_piece(RY, k), relay_piece(RY, k), stream_sem.at[6, k], role(1))
            at = rows_of(P3 + s * piece, piece)
            receive(at, stream_sem.at[3, s])
            send(at, rows_of(P3O + s * piece, piece), stream_sem.at[4, s], mate)
            if s % (2 * per_unit) == 2 * per_unit - 1:
                at = P3 + (s + 1) * piece - 2 * unit_rows
                pairs(OWN, 2 * n, at, (at, at + unit_rows))
            if s % per_unit == per_unit - 1:
                u = s // per_unit - (units - early)
                if u >= 0:
                    take_unit(u)
                    meet(OWN, 2 * n, u)
        for s in range(SUBS):
            receive(rows_of(P3O + s * piece, piece), stream_sem.at[4, s])
        for u in range(early):
            meet(P3, 2 * n, u)
        for u in range(early, units):
            take_unit(u)
            meet(OWN, 4 * n, u)
        send_result(0, column_result(P0), 2, role(0))
        send_result(1, column_result(P1), 2, role(1))
        send_result(2, jnp.maximum(column_result(P3), row_result(P3)), 1, role(3))
        send_result(3, row_result(P3O), 2, role(3, True))
        send_result(4, row_result(MATE), 0, mate)
        best = row_result(OWN)
        put(jnp.maximum(best, take_result(0)))
        finish()


def hub(embeddings, member_order, threshold):
    n, width = embeddings.shape
    vmem = pl.BlockSpec(memory_space=pltpu.VMEM)
    best = pl.pallas_call(
        hub_kernel,
        out_shape=jax.ShapeDtypeStruct((1, n), jnp.float32),
        in_specs=[vmem, vmem],
        out_specs=vmem,
        scratch_shapes=[
            pltpu.VMEM((6 * n, width), jnp.bfloat16),
            pltpu.VMEM((n, width), jnp.bfloat16),
            pltpu.VMEM((1, 6 * n), jnp.int32),
            pltpu.VMEM((4 * n, LANES), jnp.int32),
            pltpu.VMEM((4 * n, LANES), jnp.float32),
            pltpu.VMEM((8, 6 * n), jnp.float32),
            pltpu.VMEM((5, 1, n), jnp.float32),
            pltpu.VMEM((3, 1, n), jnp.float32),
            pltpu.SemaphoreType.DMA((6 * SUBS + 16,)),
            pltpu.SemaphoreType.DMA((7, SUBS)),
            pltpu.SemaphoreType.DMA((11,)),
        ],
        compiler_params=pltpu.CompilerParams(collective_id=0, has_side_effects=True),
    )(embeddings, member_order.reshape(1, n))
    best = jnp.maximum(best.reshape(n), jnp.float32(-1.0))
    return best, jnp.maximum(best - threshold[0], jnp.float32(0.0))


def solution(mesh):
    lines = mesh.shape["clusters"] == 4 and mesh.shape["members"] == 8
    placed = (P(("clusters", "members"), None), P(("clusters", "members")), P("clusters"))
    return jax.shard_map(
        hub if lines else ring,
        mesh=mesh,
        in_specs=placed,
        out_specs=(P(("clusters", "members")), P(("clusters", "members"))),
        check_vma=False,
    )
```

```python
import jax
import jax.numpy as jnp
from jax import lax
from jax.experimental import pallas as pl
from jax.experimental.pallas import tpu as pltpu
from jax.sharding import PartitionSpec as P

MESH = pl.DeviceIdType.MESH
LANES = 128
SUBS = 8
DIRECT = 1
TILE = 512


def from_behind(array, axis, by):
    size = lax.axis_size(axis)
    return lax.ppermute(array, axis, [(i, (i + by) % size) for i in range(size)])


def block_scores(unit, other):
    return lax.dot_general(
        unit, other, (((1,), (1,)), ((), ())), preferred_element_type=jnp.float32
    )


def ring(embeddings, member_order, threshold):
    unit = (
        embeddings * lax.rsqrt(jnp.sum(embeddings * embeddings, axis=1, keepdims=True) + 1e-06)
    ).astype(jnp.bfloat16)
    floor_value = jnp.float32(-1.0)
    start_best = jnp.full((unit.shape[0],), -1.0, jnp.float32)
    steps_half = lax.axis_size("members") // 2
    scores = block_scores(unit, unit)
    mask = member_order[None, :] < member_order[:, None]
    best = jnp.maximum(start_best, jnp.max(jnp.where(mask, scores, floor_value), axis=1))

    def one_step(step, carry):
        held_unit, held_order, column_best, row_best = carry
        held_unit, held_order = from_behind((held_unit, held_order), "members", 1)
        column_best = from_behind(column_best, "members", 1)
        scores = block_scores(unit, held_unit)
        row_mask = held_order[None, :] < member_order[:, None]
        row_best = jnp.maximum(row_best, jnp.max(jnp.where(row_mask, scores, floor_value), axis=1))
        column_mask = member_order[:, None] < held_order[None, :]
        column_best = jnp.maximum(
            column_best, jnp.max(jnp.where(column_mask, scores, floor_value), axis=0)
        )
        return (held_unit, held_order, column_best, row_best)

    carry = (unit, member_order, start_best, best)
    carry = lax.fori_loop(0, steps_half, one_step, carry)
    returned = from_behind(carry[2], "members", -steps_half)
    best = jnp.maximum(carry[3], returned)
    excess = jnp.maximum(best - threshold[0], jnp.float32(0.0))
    return (best, excess)


def hub_kernel(emb, order, best_out, held, relay, order_row, order_column,
               row_best, column_best, stage, arrived, rows_in, load_sem, send_sem, stream_sem, small_sem):
    n = emb.shape[0]
    half = n // 2
    piece = n // SUBS
    unit_rows = LANES
    units = n // unit_rows
    per_unit = SUBS // units
    small = unit_rows // 2 // per_unit
    OWN, MATE, P3, P3O, P0, P1 = [i * n for i in range(6)]
    MEET = P0
    RX, RY = 0, half

    cluster = lax.axis_index("clusters")
    member = lax.axis_index("members")
    members = lax.axis_size("members")
    chips = members // 2
    core = lax.rem(member, 2)
    z = member // 2
    cx = lax.rem(cluster, 2)
    cy = cluster // 2
    flip = lax.rem(cx + cy, 2)
    p = z + flip * (chips - 1 - 2 * z)
    x_peer = (cluster + 1 - 2 * cx, member)
    y_peer = (cluster + 2 - 4 * cy, member)

    def role(r, other_core=False):
        zz = r + flip * (chips - 1 - 2 * r)
        cc = 1 - core if other_core else core
        return (cluster, zz * 2 + cc)

    mate = (cluster, z * 2 + 1 - core)

    barrier = pltpu.get_barrier_semaphore()
    greets = (
        (mate, role(1), role(2)),
        (mate, role(0), role(2), x_peer, y_peer),
        (mate, role(0), role(1), role(3), role(3, True), x_peer, y_peer),
        (mate, role(2), role(2, True)),
    )
    for r, peers in enumerate(greets):
        @pl.when(p == r)
        def _():
            for peer in peers:
                pl.semaphore_signal(barrier, inc=1, device_id=peer, device_id_type=MESH)

    loads = []
    for i in range(n // LANES):
        rows = pl.ds(i * LANES, LANES)
        loads.append(pltpu.make_async_copy(emb.at[rows, :], rows_in.at[rows, :], load_sem.at[i]))
        loads[-1].start()

    order_row[:, pl.ds(OWN, n)] = order[...]
    row_best[...] = jnp.full(row_best.shape, -1.0, jnp.float32)
    column_best[...] = jnp.full(column_best.shape, -1.0, jnp.float32)

    def put_order_column(at):
        o = order_row[:, pl.ds(at, n)]
        order_column[pl.ds(at, n), :] = jnp.broadcast_to(o, (LANES, n)).T

    put_order_column(OWN)

    for i, load in enumerate(loads):
        load.wait()

        def normalise(j, _):
            rows = pl.ds(pl.multiple_of(i * LANES + j * 64, 64), 64)
            e = rows_in[rows, :]
            total = jnp.sum(e * e, axis=1, keepdims=True)
            held[rows, :] = (e * lax.rsqrt(total + 1e-06)).astype(jnp.bfloat16)
            return 0

        lax.fori_loop(0, LANES // 64, normalise, 0)

    for r, peers in enumerate(greets):
        @pl.when(p == r)
        def _():
            pl.semaphore_wait(barrier, len(peers))

    sent = []

    def send(src, dst, sem, peer):
        copy = pltpu.make_async_remote_copy(
            src_ref=src, dst_ref=dst, send_sem=send_sem.at[len(sent)], recv_sem=sem,
            device_id=peer, device_id_type=MESH,
        )
        copy.start()
        sent.append(copy)

    def receive(dst, sem):
        pltpu.make_async_remote_copy(
            src_ref=dst, dst_ref=dst, send_sem=send_sem.at[0], recv_sem=sem,
            device_id=mate, device_id_type=MESH,
        ).wait_recv()

    def rows_of(at, size):
        return held.at[pl.ds(at, size), :]

    def orders_of(at):
        return order_row.at[:, pl.ds(at, n)]

    def send_order(to, sem_index, peer):
        send(orders_of(OWN), orders_of(to), small_sem.at[sem_index], peer)

    def receive_order(at, sem_index):
        receive(orders_of(at), small_sem.at[sem_index])

    def finish():
        for copy in sent:
            copy.wait_send()
        sent.clear()

    def pairs(row0, rows, col0, members_at, columns_too=True):
        def one(i, _):
            r = pl.ds(pl.multiple_of(row0 + i * TILE, TILE), TILE)
            s = block_scores(held[r, :], held[pl.ds(col0, len(members_at) * LANES), :])
            oc = order_column[r, :]
            best = row_best[r, :]
            for c, at in enumerate(members_at):
                part = s[:, c * LANES:(c + 1) * LANES]
                at = pl.ds(at, LANES)
                earlier = order_row[:, at] < oc
                best = jnp.maximum(best, jnp.where(earlier, part, -1.0))
                if columns_too:
                    other = jnp.where(earlier, -1.0, part).reshape(TILE // 8, 8, LANES)
                    column_best[:, at] = jnp.maximum(column_best[:, at], jnp.max(other, axis=0))
            row_best[r, :] = best
            return 0

        lax.fori_loop(0, rows // TILE, one, 0)

    def meet(row0, rows, u):
        pairs(row0, rows, MEET + 2 * u * unit_rows, (P0 + u * unit_rows, P1 + u * unit_rows))

    def row_result(at):
        return jnp.max(row_best[pl.ds(at, n), :].T, axis=0, keepdims=True)

    def column_result(at):
        return jnp.max(column_best[:, pl.ds(at, n)], axis=0, keepdims=True)

    def send_result(slot, value, to, peer):
        stage[slot] = value
        send(stage.at[slot], arrived.at[to], small_sem.at[8 + to], peer)

    def take_result(slot):
        receive(arrived.at[slot], small_sem.at[8 + slot])
        return arrived[slot]

    def put(best):
        best_out[...] = best

    def exchange():
        send_order(MATE, 0, mate)
        send(rows_of(OWN, n), rows_of(MATE, n), small_sem.at[5], mate)

    def local():
        for c in range(0, n, 2 * LANES):
            pairs(OWN, n, OWN + c, (OWN + c, OWN + c + LANES), False)
        receive_order(MATE, 0)
        receive(rows_of(MATE, n), small_sem.at[5])
        for c in range(0, n, 2 * LANES):
            pairs(OWN, n, MATE + c, (MATE + c, MATE + c + LANES), False)

    def x_rows(s):
        return (s // per_unit) * unit_rows + (s % per_unit) * small

    def y_rows(s):
        return x_rows(s) + unit_rows // 2

    def p0_piece(s):
        at = s * piece
        return rows_of(MEET + 2 * (at - at % unit_rows) + at % unit_rows, piece)

    def p1_piece(at):
        return rows_of(MEET + 2 * (at - at % unit_rows) + unit_rows + at % unit_rows, small)

    @pl.when(p == 0)
    def _():
        send_order(P0, 1, role(1))
        send_order(P0, 1, role(2))
        for s in range(SUBS):
            send(rows_of(OWN + s * piece, piece), p0_piece(s), stream_sem.at[0, s], role(1))
        exchange()
        local()
        best = row_result(OWN)
        best = jnp.maximum(best, take_result(1))
        put(jnp.maximum(best, take_result(2)))
        finish()

    @pl.when(p == 3)
    def _():
        send_order(P3, 3, role(2))
        send_order(P3O, 4, role(2, True))
        for s in range(SUBS):
            send(rows_of(OWN + s * piece, piece), rows_of(P3 + s * piece, piece), stream_sem.at[3, s], role(2))
        exchange()
        local()
        best = row_result(OWN)
        best = jnp.maximum(best, take_result(1))
        put(jnp.maximum(best, take_result(2)))
        finish()

    def relay_piece(base, s):
        return relay.at[pl.ds(base + s * small, small), :]

    @pl.when(p == 1)
    def _():
        send_order(P1, 2, role(2))
        for s in range(DIRECT):
            send(rows_of(OWN + x_rows(s), small), p1_piece(x_rows(s)), stream_sem.at[1, s], role(2))
            send(rows_of(OWN + y_rows(s), small), p1_piece(y_rows(s)), stream_sem.at[2, s], role(2))
        for s in range(DIRECT, SUBS):
            send(rows_of(OWN + x_rows(s), small), relay_piece(RX, s), stream_sem.at[5, s], x_peer)
            send(rows_of(OWN + y_rows(s), small), relay_piece(RY, s), stream_sem.at[6, s], y_peer)
        exchange()
        local()
        put_order_column(MATE)
        receive_order(P0, 1)
        lag = 1
        for s in range(SUBS + lag):
            if s < SUBS:
                at = p0_piece(s)
                receive(at, stream_sem.at[0, s])
                send(at, at, stream_sem.at[0, s], role(2))
            if s >= lag:
                k = s - lag
                if k >= DIRECT:
                    receive(relay_piece(RX, k), stream_sem.at[5, k])
                    send(relay_piece(RX, k), p1_piece(x_rows(k)), stream_sem.at[1, k], x_peer)
                    receive(relay_piece(RY, k), stream_sem.at[6, k])
                    send(relay_piece(RY, k), p1_piece(y_rows(k)), stream_sem.at[2, k], y_peer)
                if k % per_unit == per_unit - 1:
                    u = k // per_unit
                    at = P0 + u * unit_rows
                    pairs(OWN, 2 * n, MEET + 2 * u * unit_rows, (at,))
        send_result(0, row_result(MATE), 0, mate)
        send_result(1, column_result(P0), 1, role(0))
        best = row_result(OWN)
        best = jnp.maximum(best, take_result(0))
        put(jnp.maximum(best, take_result(2)))
        finish()

    @pl.when(p == 2)
    def _():
        exchange()
        local()
        put_order_column(MATE)
        receive_order(P3, 3)
        put_order_column(P3)
        receive_order(P3O, 4)
        put_order_column(P3O)
        receive_order(P0, 1)
        receive_order(P1, 2)

        def take_p0(u):
            for s in range(u * per_unit, (u + 1) * per_unit):
                receive(p0_piece(s), stream_sem.at[0, s])

        def take_p1(u):
            for s in range(u * per_unit, (u + 1) * per_unit):
                receive(p1_piece(x_rows(s)), stream_sem.at[1, s])
                receive(p1_piece(y_rows(s)), stream_sem.at[2, s])

        def take_unit(u):
            take_p0(u)
            take_p1(u)

        early = units // 2
        for s in range(SUBS):
            for k in range(max(2 * s, DIRECT), min(2 * s + 2, SUBS)):
                receive(relay_piece(RX, k), stream_sem.at[5, k])
                send(relay_piece(RX, k), relay_piece(RX, k), stream_sem.at[5, k], role(1))
                receive(relay_piece(RY, k), stream_sem.at[6, k])
                send(relay_piece(RY, k), relay_piece(RY, k), stream_sem.at[6, k], role(1))
            at = rows_of(P3 + s * piece, piece)
            receive(at, stream_sem.at[3, s])
            send(at, rows_of(P3O + s * piece, piece), stream_sem.at[4, s], mate)
            if s % (2 * per_unit) == 2 * per_unit - 1:
                at = P3 + (s + 1) * piece - 2 * unit_rows
                pairs(OWN, 2 * n, at, (at, at + unit_rows))
            if s % per_unit == per_unit - 1:
                u = s // per_unit - (units - early)
                if u >= 0:
                    take_unit(u)
                    meet(OWN, 2 * n, u)
        for s in range(SUBS):
            receive(rows_of(P3O + s * piece, piece), stream_sem.at[4, s])
        for u in range(early):
            meet(P3, 2 * n, u)
        for u in range(early, units - 1):
            take_unit(u)
            meet(OWN, 4 * n, u)
        u = units - 1
        take_p0(u)
        pairs(OWN, 4 * n, MEET + 2 * u * unit_rows, (P0 + u * unit_rows,))
        send_result(0, column_result(P0), 2, role(0))
        take_p1(u)
        pairs(OWN, 4 * n, MEET + (2 * u + 1) * unit_rows, (P1 + u * unit_rows,))
        send_result(1, column_result(P1), 2, role(1))
        send_result(2, jnp.maximum(column_result(P3), row_result(P3)), 1, role(3))
        send_result(3, row_result(P3O), 2, role(3, True))
        send_result(4, row_result(MATE), 0, mate)
        best = row_result(OWN)
        put(jnp.maximum(best, take_result(0)))
        finish()


def hub(embeddings, member_order, threshold):
    n, width = embeddings.shape
    vmem = pl.BlockSpec(memory_space=pltpu.VMEM)
    best = pl.pallas_call(
        hub_kernel,
        out_shape=jax.ShapeDtypeStruct((1, n), jnp.float32),
        in_specs=[pl.BlockSpec(memory_space=pl.ANY), vmem],
        out_specs=vmem,
        scratch_shapes=[
            pltpu.VMEM((6 * n, width), jnp.bfloat16),
            pltpu.VMEM((n, width), jnp.bfloat16),
            pltpu.VMEM((1, 6 * n), jnp.int32),
            pltpu.VMEM((4 * n, LANES), jnp.int32),
            pltpu.VMEM((4 * n, LANES), jnp.float32),
            pltpu.VMEM((8, 6 * n), jnp.float32),
            pltpu.VMEM((5, 1, n), jnp.float32),
            pltpu.VMEM((3, 1, n), jnp.float32),
            pltpu.VMEM((n, width), jnp.float32),
            pltpu.SemaphoreType.DMA((n // LANES,)),
            pltpu.SemaphoreType.DMA((6 * SUBS + 16,)),
            pltpu.SemaphoreType.DMA((7, SUBS)),
            pltpu.SemaphoreType.DMA((11,)),
        ],
        compiler_params=pltpu.CompilerParams(collective_id=0, has_side_effects=True),
    )(embeddings, member_order.reshape(1, n))
    best = jnp.maximum(best.reshape(n), jnp.float32(-1.0))
    return best, jnp.maximum(best - threshold[0], jnp.float32(0.0))


def solution(mesh):
    lines = mesh.shape["clusters"] == 4 and mesh.shape["members"] == 8
    placed = (P(("clusters", "members"), None), P(("clusters", "members")), P("clusters"))
    return jax.shard_map(
        hub if lines else ring,
        mesh=mesh,
        in_specs=placed,
        out_specs=(P(("clusters", "members")), P(("clusters", "members"))),
        check_vma=False,
    )
```

```python
import jax
import jax.numpy as jnp
from jax import lax
from jax.experimental import pallas as pl
from jax.experimental.pallas import tpu as pltpu
from jax.sharding import PartitionSpec as P

MESH = pl.DeviceIdType.MESH
LANES = 128
SUBS = 8
DIRECT = 1
TILE = 1024


def from_behind(array, axis, by):
    size = lax.axis_size(axis)
    return lax.ppermute(array, axis, [(i, (i + by) % size) for i in range(size)])


def block_scores(unit, other):
    return lax.dot_general(
        unit, other, (((1,), (1,)), ((), ())), preferred_element_type=jnp.float32
    )


def ring(embeddings, member_order, threshold):
    unit = (
        embeddings * lax.rsqrt(jnp.sum(embeddings * embeddings, axis=1, keepdims=True) + 1e-06)
    ).astype(jnp.bfloat16)
    floor_value = jnp.float32(-1.0)
    start_best = jnp.full((unit.shape[0],), -1.0, jnp.float32)
    steps_half = lax.axis_size("members") // 2
    scores = block_scores(unit, unit)
    mask = member_order[None, :] < member_order[:, None]
    best = jnp.maximum(start_best, jnp.max(jnp.where(mask, scores, floor_value), axis=1))

    def one_step(step, carry):
        held_unit, held_order, column_best, row_best = carry
        held_unit, held_order = from_behind((held_unit, held_order), "members", 1)
        column_best = from_behind(column_best, "members", 1)
        scores = block_scores(unit, held_unit)
        row_mask = held_order[None, :] < member_order[:, None]
        row_best = jnp.maximum(row_best, jnp.max(jnp.where(row_mask, scores, floor_value), axis=1))
        column_mask = member_order[:, None] < held_order[None, :]
        column_best = jnp.maximum(
            column_best, jnp.max(jnp.where(column_mask, scores, floor_value), axis=0)
        )
        return (held_unit, held_order, column_best, row_best)

    carry = (unit, member_order, start_best, best)
    carry = lax.fori_loop(0, steps_half, one_step, carry)
    returned = from_behind(carry[2], "members", -steps_half)
    best = jnp.maximum(carry[3], returned)
    excess = jnp.maximum(best - threshold[0], jnp.float32(0.0))
    return (best, excess)


def hub_kernel(emb, order, best_out, held, relay, order_row, order_column,
               row_best, column_best, stage, arrived, rows_in, load_sem, send_sem, stream_sem, small_sem):
    n = emb.shape[0]
    half = n // 2
    piece = n // SUBS
    unit_rows = LANES
    units = n // unit_rows
    per_unit = SUBS // units
    small = unit_rows // 2 // per_unit
    OWN, MATE, P3, P3O, P0, P1 = [i * n for i in range(6)]
    MEET = P0
    RX, RY = 0, half

    cluster = lax.axis_index("clusters")
    member = lax.axis_index("members")
    members = lax.axis_size("members")
    chips = members // 2
    core = lax.rem(member, 2)
    z = member // 2
    cx = lax.rem(cluster, 2)
    cy = cluster // 2
    flip = lax.rem(cx + cy, 2)
    p = z + flip * (chips - 1 - 2 * z)
    x_peer = (cluster + 1 - 2 * cx, member)
    y_peer = (cluster + 2 - 4 * cy, member)

    def role(r, other_core=False):
        zz = r + flip * (chips - 1 - 2 * r)
        cc = 1 - core if other_core else core
        return (cluster, zz * 2 + cc)

    mate = (cluster, z * 2 + 1 - core)

    barrier = pltpu.get_barrier_semaphore()
    greets = (
        (mate, role(1), role(2)),
        (mate, role(0), role(2), x_peer, y_peer),
        (mate, role(0), role(1), role(3), role(3, True), x_peer, y_peer),
        (mate, role(2), role(2, True)),
    )
    for r, peers in enumerate(greets):
        @pl.when(p == r)
        def _():
            for peer in peers:
                pl.semaphore_signal(barrier, inc=1, device_id=peer, device_id_type=MESH)

    loads = []
    for i in range(n // LANES):
        rows = pl.ds(i * LANES, LANES)
        loads.append(pltpu.make_async_copy(emb.at[rows, :], rows_in.at[rows, :], load_sem.at[i]))
        loads[-1].start()

    order_row[:, pl.ds(OWN, n)] = order[...]
    row_best[...] = jnp.full(row_best.shape, -1.0, jnp.float32)
    column_best[...] = jnp.full(column_best.shape, -1.0, jnp.float32)

    def put_order_column(at):
        o = order_row[:, pl.ds(at, n)]
        order_column[pl.ds(at, n), :] = jnp.broadcast_to(o, (LANES, n)).T

    put_order_column(OWN)

    for i, load in enumerate(loads):
        load.wait()

        def normalise(j, _):
            rows = pl.ds(pl.multiple_of(i * LANES + j * 64, 64), 64)
            e = rows_in[rows, :]
            total = jnp.sum(e * e, axis=1, keepdims=True)
            held[rows, :] = (e * lax.rsqrt(total + 1e-06)).astype(jnp.bfloat16)
            return 0

        lax.fori_loop(0, LANES // 64, normalise, 0)

    for r, peers in enumerate(greets):
        @pl.when(p == r)
        def _():
            pl.semaphore_wait(barrier, len(peers))

    sent = []

    def send(src, dst, sem, peer):
        copy = pltpu.make_async_remote_copy(
            src_ref=src, dst_ref=dst, send_sem=send_sem.at[len(sent)], recv_sem=sem,
            device_id=peer, device_id_type=MESH,
        )
        copy.start()
        sent.append(copy)

    def receive(dst, sem):
        pltpu.make_async_remote_copy(
            src_ref=dst, dst_ref=dst, send_sem=send_sem.at[0], recv_sem=sem,
            device_id=mate, device_id_type=MESH,
        ).wait_recv()

    def rows_of(at, size):
        return held.at[pl.ds(at, size), :]

    def orders_of(at):
        return order_row.at[:, pl.ds(at, n)]

    def send_order(to, sem_index, peer):
        send(orders_of(OWN), orders_of(to), small_sem.at[sem_index], peer)

    def receive_order(at, sem_index):
        receive(orders_of(at), small_sem.at[sem_index])

    def finish():
        for copy in sent:
            copy.wait_send()
        sent.clear()

    def pairs(row0, rows, col0, members_at, columns_too=True):
        def one(i, _):
            r = pl.ds(pl.multiple_of(row0 + i * min(TILE, rows), min(TILE, rows)), min(TILE, rows))
            s = block_scores(held[r, :], held[pl.ds(col0, len(members_at) * LANES), :])
            oc = order_column[r, :]
            best = row_best[r, :]
            for c, at in enumerate(members_at):
                part = s[:, c * LANES:(c + 1) * LANES]
                at = pl.ds(at, LANES)
                earlier = order_row[:, at] < oc
                best = jnp.maximum(best, jnp.where(earlier, part, -1.0))
                if columns_too:
                    other = jnp.where(earlier, -1.0, part).reshape(min(TILE, rows) // 8, 8, LANES)
                    column_best[:, at] = jnp.maximum(column_best[:, at], jnp.max(other, axis=0))
            row_best[r, :] = best
            return 0

        lax.fori_loop(0, rows // min(TILE, rows), one, 0)

    def meet(row0, rows, u):
        pairs(row0, rows, MEET + 2 * u * unit_rows, (P0 + u * unit_rows, P1 + u * unit_rows))

    def row_result(at):
        return jnp.max(row_best[pl.ds(at, n), :].T, axis=0, keepdims=True)

    def column_result(at):
        return jnp.max(column_best[:, pl.ds(at, n)], axis=0, keepdims=True)

    def send_result(slot, value, to, peer):
        stage[slot] = value
        send(stage.at[slot], arrived.at[to], small_sem.at[8 + to], peer)

    def take_result(slot):
        receive(arrived.at[slot], small_sem.at[8 + slot])
        return arrived[slot]

    def put(best):
        best_out[...] = best

    def exchange():
        send_order(MATE, 0, mate)
        send(rows_of(OWN, n), rows_of(MATE, n), small_sem.at[5], mate)

    def local():
        for c in range(0, n, 2 * LANES):
            pairs(OWN, n, OWN + c, (OWN + c, OWN + c + LANES), False)
        receive_order(MATE, 0)
        receive(rows_of(MATE, n), small_sem.at[5])
        for c in range(0, n, 2 * LANES):
            pairs(OWN, n, MATE + c, (MATE + c, MATE + c + LANES), False)

    def x_rows(s):
        return (s // per_unit) * unit_rows + (s % per_unit) * small

    def y_rows(s):
        return x_rows(s) + unit_rows // 2

    def p0_piece(s):
        at = s * piece
        return rows_of(MEET + 2 * (at - at % unit_rows) + at % unit_rows, piece)

    def p1_piece(at):
        return rows_of(MEET + 2 * (at - at % unit_rows) + unit_rows + at % unit_rows, small)

    @pl.when(p == 0)
    def _():
        send_order(P0, 1, role(1))
        send_order(P0, 1, role(2))
        for s in range(SUBS):
            send(rows_of(OWN + s * piece, piece), p0_piece(s), stream_sem.at[0, s], role(1))
        exchange()
        local()
        best = row_result(OWN)
        best = jnp.maximum(best, take_result(1))
        put(jnp.maximum(best, take_result(2)))
        finish()

    @pl.when(p == 3)
    def _():
        send_order(P3, 3, role(2))
        send_order(P3O, 4, role(2, True))
        for s in range(SUBS):
            send(rows_of(OWN + s * piece, piece), rows_of(P3 + s * piece, piece), stream_sem.at[3, s], role(2))
        exchange()
        local()
        best = row_result(OWN)
        best = jnp.maximum(best, take_result(1))
        put(jnp.maximum(best, take_result(2)))
        finish()

    def relay_piece(base, s):
        return relay.at[pl.ds(base + s * small, small), :]

    @pl.when(p == 1)
    def _():
        send_order(P1, 2, role(2))
        for s in range(DIRECT):
            send(rows_of(OWN + x_rows(s), small), p1_piece(x_rows(s)), stream_sem.at[1, s], role(2))
            send(rows_of(OWN + y_rows(s), small), p1_piece(y_rows(s)), stream_sem.at[2, s], role(2))
        for s in range(DIRECT, SUBS):
            send(rows_of(OWN + x_rows(s), small), relay_piece(RX, s), stream_sem.at[5, s], x_peer)
            send(rows_of(OWN + y_rows(s), small), relay_piece(RY, s), stream_sem.at[6, s], y_peer)
        exchange()
        local()
        put_order_column(MATE)
        receive_order(P0, 1)
        lag = 1
        for s in range(SUBS + lag):
            if s < SUBS:
                at = p0_piece(s)
                receive(at, stream_sem.at[0, s])
                send(at, at, stream_sem.at[0, s], role(2))
            if s >= lag:
                k = s - lag
                if k >= DIRECT:
                    receive(relay_piece(RX, k), stream_sem.at[5, k])
                    send(relay_piece(RX, k), p1_piece(x_rows(k)), stream_sem.at[1, k], x_peer)
                    receive(relay_piece(RY, k), stream_sem.at[6, k])
                    send(relay_piece(RY, k), p1_piece(y_rows(k)), stream_sem.at[2, k], y_peer)
                if k % per_unit == per_unit - 1:
                    u = k // per_unit
                    at = P0 + u * unit_rows
                    pairs(OWN, 2 * n, MEET + 2 * u * unit_rows, (at,))
        send_result(0, row_result(MATE), 0, mate)
        send_result(1, column_result(P0), 1, role(0))
        best = row_result(OWN)
        best = jnp.maximum(best, take_result(0))
        put(jnp.maximum(best, take_result(2)))
        finish()

    @pl.when(p == 2)
    def _():
        exchange()
        local()
        put_order_column(MATE)
        receive_order(P3, 3)
        put_order_column(P3)
        receive_order(P3O, 4)
        put_order_column(P3O)
        receive_order(P0, 1)
        receive_order(P1, 2)

        def take_p0(u):
            for s in range(u * per_unit, (u + 1) * per_unit):
                receive(p0_piece(s), stream_sem.at[0, s])

        def take_p1(u):
            for s in range(u * per_unit, (u + 1) * per_unit):
                receive(p1_piece(x_rows(s)), stream_sem.at[1, s])
                receive(p1_piece(y_rows(s)), stream_sem.at[2, s])

        def take_unit(u):
            take_p0(u)
            take_p1(u)

        early = units // 2
        for s in range(SUBS):
            for k in range(max(2 * s, DIRECT), min(2 * s + 2, SUBS)):
                receive(relay_piece(RX, k), stream_sem.at[5, k])
                send(relay_piece(RX, k), relay_piece(RX, k), stream_sem.at[5, k], role(1))
                receive(relay_piece(RY, k), stream_sem.at[6, k])
                send(relay_piece(RY, k), relay_piece(RY, k), stream_sem.at[6, k], role(1))
            at = rows_of(P3 + s * piece, piece)
            receive(at, stream_sem.at[3, s])
            send(at, rows_of(P3O + s * piece, piece), stream_sem.at[4, s], mate)
            if s % (2 * per_unit) == 2 * per_unit - 1:
                at = P3 + (s + 1) * piece - 2 * unit_rows
                pairs(OWN, 2 * n, at, (at, at + unit_rows))
            if s % per_unit == per_unit - 1:
                u = s // per_unit - (units - early)
                if u >= 0:
                    take_unit(u)
                    meet(OWN, 2 * n, u)
        for s in range(SUBS):
            receive(rows_of(P3O + s * piece, piece), stream_sem.at[4, s])
        for u in range(early):
            meet(P3, 2 * n, u)
        for u in range(early, units - 1):
            take_unit(u)
            meet(OWN, 4 * n, u)
        u = units - 1
        take_p0(u)
        pairs(OWN, 4 * n, MEET + 2 * u * unit_rows, (P0 + u * unit_rows,))
        send_result(0, column_result(P0), 2, role(0))
        take_p1(u)
        pairs(OWN, 4 * n, MEET + (2 * u + 1) * unit_rows, (P1 + u * unit_rows,))
        send_result(1, column_result(P1), 2, role(1))
        send_result(2, jnp.maximum(column_result(P3), row_result(P3)), 1, role(3))
        send_result(3, row_result(P3O), 2, role(3, True))
        send_result(4, row_result(MATE), 0, mate)
        best = row_result(OWN)
        put(jnp.maximum(best, take_result(0)))
        finish()


def hub(embeddings, member_order, threshold):
    n, width = embeddings.shape
    vmem = pl.BlockSpec(memory_space=pltpu.VMEM)
    best = pl.pallas_call(
        hub_kernel,
        out_shape=jax.ShapeDtypeStruct((1, n), jnp.float32),
        in_specs=[pl.BlockSpec(memory_space=pl.ANY), vmem],
        out_specs=vmem,
        scratch_shapes=[
            pltpu.VMEM((6 * n, width), jnp.bfloat16),
            pltpu.VMEM((n, width), jnp.bfloat16),
            pltpu.VMEM((1, 6 * n), jnp.int32),
            pltpu.VMEM((4 * n, LANES), jnp.int32),
            pltpu.VMEM((4 * n, LANES), jnp.float32),
            pltpu.VMEM((8, 6 * n), jnp.float32),
            pltpu.VMEM((5, 1, n), jnp.float32),
            pltpu.VMEM((3, 1, n), jnp.float32),
            pltpu.VMEM((n, width), jnp.float32),
            pltpu.SemaphoreType.DMA((n // LANES,)),
            pltpu.SemaphoreType.DMA((6 * SUBS + 16,)),
            pltpu.SemaphoreType.DMA((7, SUBS)),
            pltpu.SemaphoreType.DMA((11,)),
        ],
        compiler_params=pltpu.CompilerParams(collective_id=0, has_side_effects=True),
    )(embeddings, member_order.reshape(1, n))
    best = jnp.maximum(best.reshape(n), jnp.float32(-1.0))
    return best, jnp.maximum(best - threshold[0], jnp.float32(0.0))


def solution(mesh):
    lines = mesh.shape["clusters"] == 4 and mesh.shape["members"] == 8
    placed = (P(("clusters", "members"), None), P(("clusters", "members")), P("clusters"))
    return jax.shard_map(
        hub if lines else ring,
        mesh=mesh,
        in_specs=placed,
        out_specs=(P(("clusters", "members")), P(("clusters", "members"))),
        check_vma=False,
    )
```
